32 devices in a mesh: fsdp: 4 (over y, x), tenant: 4 (over z), dp: 2 (over core).
Axes of the slice: x: 2, y: 2, z: 4, core: 2. Of those that a mesh axis runs over, the one named last changes fastest.
Arguments:
- tokens: bfloat16 [3072, 5120], P(('fsdp', 'dp'), 'tenant'), may hold values from -6 to 6
- block_tenant_index: int32 [48], P(('fsdp', 'dp')), may hold values from 0 to 7
- ranks: int32 [8], replicated, may hold values from 16 to 64, as said below
- frozen_up_weight: bfloat16 [5120, 14336], P(('fsdp', 'dp'), 'tenant'), may hold values from -0.078125 to 0.078125
- tenant_down_adapters: bfloat16 [8, 64, 5120], P('tenant'), may hold values from -0.078125 to 0.078125
- tenant_up_adapters: bfloat16 [8, 64, 14336], P('tenant'), may hold values from -0.75 to 0.75
- cotangent: bfloat16 [3072, 14336], P(('fsdp', 'dp'), 'tenant'), may hold values from -6 to 6
Outputs:
- hidden_out: bfloat16 [3072, 14336], P(('fsdp', 'dp'), 'tenant')
- grad_tokens: bfloat16 [3072, 5120], P(('fsdp', 'dp'), 'tenant')
- grad_down: float32 [8, 64, 5120], P('dp', None, 'tenant')
- grad_up: float32 [8, 64, 14336], P('dp', None, 'tenant')
The draws below stay inside these ranges and needn't reach their ends.
Inputs may be any that keep to these rules, and one draw needn't show every extreme that they name: `ranks`: multiples of 16; some tenant has rank 64.
All inputs are finite; a program needn't handle non-finite values.
Results may differ from the reference program's by a relative error of at most 0.0034.
Values may be sent and summed in bfloat16 or wider, within the bound.
No kernel may reach another device: no remote copies, remote signals or barrier semaphores. Data moves between devices by JAX's collectives and lax.ppermute only.
A program may use at most 128 MiB of HBM per device.

```python
import math
import jax
import jax.numpy as jnp
import numpy as np

MODEL_WIDTH = 5120
HIDDEN_UNITS = 14336
TENANT_COUNT = 8
ADAPTER_RANK = 64
BLOCK = 64
TOKENS = 3072
BLOCKS = 48


def draw_ranks(key, part):
    levels = jax.random.randint(key, (TENANT_COUNT,), 1, ADAPTER_RANK // 16 + 1)
    chosen = jax.random.randint(jax.random.fold_in(key, 7), (), 0, TENANT_COUNT)
    levels = jnp.where(jnp.arange(TENANT_COUNT) == chosen, ADAPTER_RANK // 16, levels)
    return (levels * 16).astype(jnp.int32)


def place_ends(drawn, key, least, high):
    place = [jax.random.randint(jax.random.fold_in(key, axis), (), 0, length) for axis, length in enumerate(drawn.shape)]
    main_axis = drawn.shape.index(max(drawn.shape))
    next_to = place[:main_axis] + [(place[main_axis] + 1) % drawn.shape[main_axis]] + place[main_axis + 1:]
    return drawn.at[tuple(place)].set(least).at[tuple(next_to)].set(high)


def shard_levels(key, extent, shards, smallest, top_value):
    factor_of = 1.0
    for dim, blocks in shards:
        steps = jax.random.uniform(jax.random.fold_in(jax.random.fold_in(key, 6), dim), (blocks,), jnp.float32, smallest / len(shards), top_value / len(shards))
        factor_of = factor_of * jnp.repeat(jnp.exp(steps), extent[dim] // blocks).reshape((-1,) + (1,) * (len(extent) - 1 - dim))
    return factor_of


def rank_table(number_of, lean):
    weights = [(1 << 20) // math.isqrt(grade ** lean) + 1 for grade in range(1, number_of + 1)]
    deviation = 1 + sum(weights) // (1 << 30)
    return np.cumsum(np.array([max(1, weight // deviation) for weight in weights]))


def ranked(stream_key, extent, number_of, skew):
    grid = rank_table(number_of, skew)
    pick = jax.random.randint(jax.random.fold_in(stream_key, 1), extent, 0, int(grid[number_of - 1]))
    rank = jnp.searchsorted(jnp.asarray(grid, jnp.int32), pick, side="right")
    return jax.random.permutation(jax.random.fold_in(stream_key, 2), number_of)[rank].astype(jnp.int32)


def centred(stream_key, extent, spread, most, shards=(), kind=jnp.bfloat16):
    result = spread * jax.random.normal(stream_key, extent, jnp.float32)
    if shards:
        result = result * shard_levels(stream_key, extent, shards, -0.22, 0.18)
    return jnp.clip(result, -most, most).astype(kind)


def setup_inputs(seed: int = 0) -> dict:
    splits = jax.random.split(jax.random.key(seed), 8)
    return {
        "tokens": centred(splits[0], (TOKENS, MODEL_WIDTH), 1.0, 6.0, ((0, 8), (1, 4))),
        "block_tenant_index": place_ends(ranked(splits[1], (BLOCKS,), TENANT_COUNT, 2), jax.random.fold_in(splits[1], 3), 0, TENANT_COUNT - 1).astype(jnp.int32),
        "ranks": draw_ranks(jax.random.fold_in(splits[7], 71), 0),
        "frozen_up_weight": centred(splits[3], (MODEL_WIDTH, HIDDEN_UNITS), MODEL_WIDTH ** -0.5, 0.078125, ((0, 8), (1, 4))),
        "tenant_down_adapters": centred(splits[4], (TENANT_COUNT, ADAPTER_RANK, MODEL_WIDTH), MODEL_WIDTH ** -0.5, 0.078125, ((0, 4),)),
        "tenant_up_adapters": centred(splits[5], (TENANT_COUNT, ADAPTER_RANK, HIDDEN_UNITS), ADAPTER_RANK ** -0.5, 0.75, ((0, 4),)),
        "cotangent": centred(splits[6], (TOKENS, HIDDEN_UNITS), 1.0, 6.0, ((0, 8), (1, 4))),
    }


alpha_scale = 32.0


def make_gain(block_tenant_index, ranks):
    rows_tenant = jnp.repeat(block_tenant_index, BLOCK, total_repeat_length=TOKENS)
    columns = jnp.arange(TENANT_COUNT * ADAPTER_RANK, dtype=jnp.int32)
    col_tenant = columns // ADAPTER_RANK
    col_slot = columns % ADAPTER_RANK
    ranks_col = jnp.repeat(ranks, ADAPTER_RANK, total_repeat_length=TENANT_COUNT * ADAPTER_RANK)
    keep = (rows_tenant[:, None] == col_tenant[None, :]) & (col_slot[None, :] < ranks_col[None, :])
    scale_col = alpha_scale / ranks_col.astype(jnp.float32)
    return jnp.where(keep, scale_col[None, :], jnp.float32(0.0))


def reference(tokens, block_tenant_index, ranks, frozen_up_weight, tenant_down_adapters, tenant_up_adapters, cotangent):
    gain = make_gain(block_tenant_index, ranks)
    flattened_down = tenant_down_adapters.reshape(TENANT_COUNT * ADAPTER_RANK, MODEL_WIDTH)
    flattened_up = tenant_up_adapters.reshape(TENANT_COUNT * ADAPTER_RANK, HIDDEN_UNITS)
    proj = jnp.dot(tokens, flattened_down.T, preferred_element_type=jnp.float32)
    adapted = (proj * gain).astype(jnp.bfloat16)
    base = jnp.dot(tokens, frozen_up_weight, preferred_element_type=jnp.float32)
    hidden_out = (base + jnp.dot(adapted, flattened_up, preferred_element_type=jnp.float32)).astype(jnp.bfloat16)
    back = jnp.dot(cotangent, flattened_up.T, preferred_element_type=jnp.float32)
    adapted_grad = (back * gain).astype(jnp.bfloat16)
    grad_base = jnp.dot(cotangent, frozen_up_weight.T, preferred_element_type=jnp.float32)
    grad_tokens = (grad_base + jnp.dot(adapted_grad, flattened_down, preferred_element_type=jnp.float32)).astype(jnp.bfloat16)
    grad_up = jnp.dot(adapted.T, cotangent, preferred_element_type=jnp.float32).reshape(TENANT_COUNT, ADAPTER_RANK, HIDDEN_UNITS)
    grad_down = jnp.dot(adapted_grad.T, tokens, preferred_element_type=jnp.float32).reshape(TENANT_COUNT, ADAPTER_RANK, MODEL_WIDTH)
    return hidden_out, grad_tokens, grad_down, grad_up
```

```python
import math

import jax
import jax.numpy as jnp
from jax import lax
from jax.experimental import pallas as pl
from jax.experimental.pallas import tpu as pltpu
from jax.sharding import PartitionSpec as P


BLOCK = 64
alpha_scale = 32.0
BF16 = jnp.bfloat16
F32 = jnp.float32


def flip(x, axis, n, s):
    return lax.ppermute(x, axis, [(i, i ^ s) for i in range(n)])


def dot(a, b, ca, cb):
    return lax.dot_general(a, b, (((ca,), (cb,)), ((), ())), preferred_element_type=F32)


def sum_of_dots(pairs, dtype):
    rows, cols = pairs[0][0].shape[0], pairs[0][1].shape[1]
    tile = next(t for t in (512, 256, 128) if cols % t == 0)
    count = len(pairs)

    def kernel(*refs):
        total = None
        for k in range(count):
            part = jnp.dot(refs[k][...], refs[count + k][...], preferred_element_type=F32)
            total = part if total is None else total + part
        refs[-1][...] = total.astype(dtype)

    depth = sum(a.shape[1] for a, _ in pairs)
    specs = [pl.BlockSpec(a.shape, lambda i: (0, 0)) for a, _ in pairs]
    specs += [pl.BlockSpec((b.shape[0], tile), lambda i: (0, i)) for _, b in pairs]
    return pl.pallas_call(
        kernel,
        grid=(cols // tile,),
        in_specs=specs,
        out_specs=pl.BlockSpec((rows, tile), lambda i: (0, i)),
        out_shape=jax.ShapeDtypeStruct((rows, cols), dtype),
        compiler_params=pltpu.CompilerParams(
            dimension_semantics=("arbitrary",), vmem_limit_bytes=48 * 1024 * 1024
        ),
        cost_estimate=pl.CostEstimate(
            flops=2 * rows * cols * depth,
            bytes_accessed=2 * depth * (rows + cols) + 2 * rows * cols,
            transcendentals=0,
        ),
    )(*[a for a, _ in pairs], *[b for _, b in pairs])


def input_grads(places, cot_t, grad, down, mine, other, nt, block_rows, begin):
    depth, rows = cot_t.shape
    part = mine.shape[0] // nt
    rank = grad.shape[1]
    step = math.gcd(block_rows, begin) if begin else block_rows
    whole_tile = step % 128 == 0

    def kernel(at, cot_ref, grad_ref, down_ref, mine_ref, other_ref, *outs):
        r = pl.program_id(0)
        for h, w_ref in enumerate((mine_ref, other_ref)):
            if whole_tile:
                start = pl.multiple_of(at[2 * nt + h] * block_rows + begin, 128)
                d = down_ref[:, pl.ds(start, part)]
            else:
                d = down_ref[h, 0]
            g = jnp.dot(w_ref[...], cot_ref[...], preferred_element_type=F32)
            g = g.T + jnp.dot(grad_ref[...], d, preferred_element_type=F32)
            for k in range(nt):

                @pl.when(r == k)
                def _(k=k, g=g, h=h):
                    outs[k][h] = g.astype(outs[k].dtype)

    if whole_tile:
        down_spec = pl.BlockSpec((rank, down.shape[1] // nt), lambda r, at: (0, at[nt + r]))
    else:
        cut = [
            lax.dynamic_slice(
                down.reshape(rank, nt, -1),
                (0, 0, places[2 * nt + h] * block_rows + begin),
                (rank, nt, part),
            )
            for h in range(2)
        ]
        down = jnp.stack(cut).transpose(0, 2, 1, 3)
        down_spec = pl.BlockSpec((2, 1, rank, part), lambda r, at: (0, at[nt + r], 0, 0))
    return pl.pallas_call(
        kernel,
        grid_spec=pltpu.PrefetchScalarGridSpec(
            num_scalar_prefetch=1,
            grid=(nt,),
            in_specs=[
                pl.BlockSpec((depth, rows), lambda r, at: (0, 0)),
                pl.BlockSpec((rows, rank), lambda r, at: (0, 0)),
                down_spec,
                pl.BlockSpec((part, depth), lambda r, at: (at[r], 0)),
                pl.BlockSpec((part, depth), lambda r, at: (at[r], 0)),
            ],
            out_specs=[pl.BlockSpec((2, rows, part), lambda r, at: (0, 0, 0))] * nt,
        ),
        out_shape=[
            jax.ShapeDtypeStruct((2, rows, part), F32 if k == 0 else BF16) for k in range(nt)
        ],
        compiler_params=pltpu.CompilerParams(
            dimension_semantics=("arbitrary",), vmem_limit_bytes=48 * 1024 * 1024
        ),
        cost_estimate=pl.CostEstimate(
            flops=4 * rows * (depth + rank) * mine.shape[0],
            bytes_accessed=2 * depth * (rows + 2 * mine.shape[0]) + 10 * rows * mine.shape[0],
            transcendentals=0,
        ),
    )(places, cot_t, grad, down, mine, other)


def gathered(x, n, bits):
    have = [(0, x)]
    size = x.shape[0]
    for b in bits:
        sent = jnp.concatenate([v for _, v in have], axis=0) if len(have) > 1 else x
        got = flip(sent, "fsdp", n, b)
        have = have + [
            (s | b, got[size * i : size * (i + 1)]) for i, (s, _) in enumerate(have)
        ]
    return dict(have)


def make_shards(nf, nt, nc):
    bits = [1 << k for k in range(nf.bit_length() - 1)]

    def shards(tokens, block_tenant_index, ranks, weight, down, up, cotangent):
        rows, local_d = tokens.shape
        local_f = cotangent.shape[1]
        own_tenants, largest_rank, _ = down.shape
        tenants = ranks.shape[0]
        block_rows = weight.shape[0]
        unit = block_rows // 5
        parts = (2 * unit, 2 * unit, block_rows - 4 * unit)
        begins = (0, 2 * unit, 4 * unit)
        pairs = len(parts)
        half_rank = largest_rank // 2
        f = lax.axis_index("fsdp")
        j = lax.axis_index("tenant")
        c = lax.axis_index("dp")

        row_tenant = jnp.broadcast_to(
            block_tenant_index[:, None], (block_tenant_index.shape[0], BLOCK)
        ).reshape(rows, 1)
        tenant_ids = jnp.arange(tenants, dtype=jnp.int32)[None, :]
        row_rank = jnp.sum(
            jnp.where(row_tenant == tenant_ids, ranks[None, :], 0), axis=1, keepdims=True
        )
        slots = jnp.arange(largest_rank, dtype=jnp.int32)[None, :]
        gain = jnp.where(slots < row_rank, alpha_scale / row_rank.astype(F32), F32(0.0))

        w_mine = []
        for p in range(pairs):
            half = parts[p] // 2
            got = [
                gathered(
                    weight[begins[p] + half * q : begins[p] + half * (q + 1)],
                    nf,
                    bits[::-1] if q else bits,
                )
                for q in range(2)
            ]
            w_mine.append(
                jnp.concatenate([got[q][s] for s in range(nf) for q in range(2)], axis=0)
            )
        w_other = [flip(w, "dp", nc, 1) for w in w_mine]

        def up_block(r):
            return lax.dynamic_slice(
                up, (0, c * half_rank, (j ^ r) * local_f), (own_tenants, half_rank, local_f)
            ).reshape(own_tenants * half_rank, local_f)

        up_mine = jnp.concatenate(
            [up_block(0)]
            + [flip(up_block(r), "tenant", nt, r) for r in range(1, nt)],
            axis=0,
        )
        up_other = flip(up_mine, "dp", nc, 1)

        tiles = [tokens] + [flip(tokens, "tenant", nt, r) for r in range(1, nt)]
        whole = jnp.zeros((rows, nf * local_d), BF16)
        for r in range(nt):
            whole = lax.dynamic_update_slice(whole, tiles[r], (0, (f ^ j ^ r) * local_d))
        own_down = down.reshape(own_tenants * largest_rank, -1)
        whole_down = jnp.concatenate(
            [
                lax.dynamic_slice(
                    own_down, (0, (f ^ s) * local_d), (own_tenants * largest_rank, local_d)
                )
                for s in range(nf)
            ],
            axis=1,
        )
        cores = (c, c ^ 1)

        def columns(x, h, p):
            return jnp.concatenate(
                [
                    lax.dynamic_slice(
                        x,
                        (0, s * local_d + cores[h] * block_rows + begins[p]),
                        (x.shape[0], parts[p]),
                    )
                    for s in range(nf)
                ],
                axis=1,
            )

        def halves(x):
            a, b = x[:, :half_rank], x[:, half_rank:]
            return jnp.where(c == 0, x, jnp.concatenate([b, a], axis=1))

        def fold(x):
            total = jnp.zeros((rows, half_rank), F32)
            for r in range(nt):
                for l in range(own_tenants):
                    at = (r * own_tenants + l) * half_rank
                    t = (j ^ r) * own_tenants + l
                    total = total + jnp.where(row_tenant == t, x[:, at : at + half_rank], 0.0)
            return total

        def line_sum(x):
            got = [flip(x, "tenant", nt, r) for r in range(1, nt)]
            for g in got:
                x = x + g
            return x

        back_parts = [dot(cotangent, u, 1, 1) for u in (up_mine, up_other)]
        back = jnp.concatenate([fold(x) for x in back_parts], axis=1)
        adapted_grad = (halves(line_sum(back)) * gain).astype(BF16)

        proj_own = dot(whole, whole_down, 1, 1)
        proj = jnp.zeros((rows, largest_rank), F32)
        for l in range(own_tenants):
            proj = proj + jnp.where(
                row_tenant == j * own_tenants + l,
                proj_own[:, l * largest_rank : (l + 1) * largest_rank],
                0.0,
            )
        adapted = (line_sum(proj) * gain).astype(BF16)

        def spread(x, ids, row):
            return jnp.concatenate([jnp.where(row == t, x, BF16(0.0)) for t in ids], axis=1)

        share = tenants // nc
        mine_ids = [c * share + k for k in range(share)]
        other_ids = [(c ^ 1) * share + k for k in range(share)]

        grad_mine = spread(adapted_grad, mine_ids, row_tenant)
        grad_other = spread(adapted_grad, other_ids, row_tenant)
        grad_own = spread(
            adapted_grad, [j * own_tenants + l for l in range(own_tenants)], row_tenant
        )
        ahead = grad_mine[:, :1] + grad_other[:, :1] + grad_own[:, :1]
        row_of_proj = row_tenant + (ahead * BF16(0.0)).astype(jnp.int32)

        def core_share(small_mine, small_other, wide):
            other = dot(small_other, wide, 0, 0)
            return dot(small_mine, wide, 0, 0) + flip(other, "dp", nc, 1)

        down_share = core_share(grad_mine, grad_other, tokens)
        adapted_mine = spread(adapted, mine_ids, row_of_proj)
        adapted_other = spread(adapted, other_ids, row_of_proj)
        up_share = core_share(adapted_mine, adapted_other, cotangent)
        size = share * largest_rank // nf

        def share_piece(r):
            return jnp.concatenate(
                [
                    lax.dynamic_slice(x, ((f ^ r) * size, 0), (size, x.shape[1]))
                    for x in (down_share, up_share)
                ],
                axis=1,
            )

        got = [flip(share_piece(r).astype(BF16), "fsdp", nf, r) for r in range(1, nf)]
        mine = share_piece(0)
        for g in got:
            mine = mine + g.astype(F32)
        mine = mine.astype(BF16)
        blocks = [mine] + [flip(mine, "fsdp", nf, r) for r in range(1, nf)]

        def in_order(at, width):
            both = jnp.stack([x[:, at : at + width] for x in blocks])
            both = both.reshape((2,) * len(bits) + both.shape[1:])
            for k, b in enumerate(bits[::-1]):
                both = jnp.where((f & b) != 0, jnp.flip(both, k), both)
            return both.reshape(share, largest_rank, width).astype(F32)

        grad_down = in_order(0, local_d)
        grad_up = in_order(local_d, local_f)

        cotangent_t = cotangent.T
        places = jnp.stack(
            [f ^ j ^ r for r in range(nt)] + [j ^ r for r in range(nt)] + list(cores)
        ).astype(jnp.int32)
        out = [[], []]
        for p in range(pairs):
            own_part, *away = input_grads(
                places, cotangent_t, grad_own, own_down, w_mine[p], w_other[p],
                nt, block_rows, begins[p],
            )
            got = [flip(away[r - 1], "tenant", nt, r) for r in range(1, nt)]
            total = own_part
            for g in got:
                total = total + g.astype(F32)
            for h in range(2):
                out[h].append(total[h].astype(BF16))
        own, other = (jnp.concatenate(o, axis=1) for o in out)
        grad_tokens = jnp.where(
            c == 0,
            jnp.concatenate([own, other], axis=1),
            jnp.concatenate([other, own], axis=1),
        )

        ids = [(j ^ r) * own_tenants + l for r in range(nt) for l in range(own_tenants)]
        ordered = halves(adapted)
        terms = [
            (spread(ordered[:, :half_rank], ids, row_of_proj), up_mine),
            (spread(ordered[:, half_rank:], ids, row_of_proj), up_other),
        ]
        for p in range(pairs):
            terms += [(columns(whole, 0, p), w_mine[p]), (columns(whole, 1, p), w_other[p])]
        hidden = sum_of_dots(terms, BF16)
        return hidden, grad_tokens, grad_down, grad_up

    return shards


def solution(mesh):
    nf, nt, nc = mesh.shape["fsdp"], mesh.shape["tenant"], mesh.shape["dp"]
    return jax.shard_map(
        make_shards(nf, nt, nc),
        mesh=mesh,
        in_specs=(
            P(("fsdp", "dp"), "tenant"),
            P(("fsdp", "dp")),
            P(),
            P(("fsdp", "dp"), "tenant"),
            P("tenant", None, None),
            P("tenant", None, None),
            P(("fsdp", "dp"), "tenant"),
        ),
        out_specs=(
            P(("fsdp", "dp"), "tenant"),
            P(("fsdp", "dp"), "tenant"),
            P("dp", None, "tenant"),
            P("dp", None, "tenant"),
        ),
        check_vma=False,
    )
```

```python
import math

import jax
import jax.numpy as jnp
from jax import lax
from jax.experimental import pallas as pl
from jax.experimental.pallas import tpu as pltpu
from jax.sharding import PartitionSpec as P


BLOCK = 64
alpha_scale = 32.0
BF16 = jnp.bfloat16
F32 = jnp.float32


def flip(x, axis, n, s):
    return lax.ppermute(x, axis, [(i, i ^ s) for i in range(n)])


def dot(a, b, ca, cb):
    return lax.dot_general(a, b, (((ca,), (cb,)), ((), ())), preferred_element_type=F32)


def hidden_sum(places, whole, begins, block_rows, nf, pairs):
    rows, cols = whole.shape[0], pairs[0][1].shape[1]
    tile = next(t for t in (512, 256, 128) if cols % t == 0)
    local_d = whole.shape[1] // nf
    lefts = [a for a, _ in pairs if a is not None]
    rights = [b for _, b in pairs]

    def kernel(at, *refs):
        left, right = list(refs[: len(lefts)]), refs[len(lefts) + 1 : -1]
        whole_ref = refs[len(lefts)]
        total = None
        for k, ((a, w), w_ref) in enumerate(zip(pairs, right)):
            if a is None:
                p, h = divmod(k - len(lefts), 2)
                part = w.shape[0] // nf
                starts = [
                    pl.multiple_of(s * local_d + at[h] * block_rows + begins[p], 128)
                    for s in range(nf)
                ]
                x = jnp.concatenate([whole_ref[:, pl.ds(b, part)] for b in starts], axis=1)
            else:
                x = left.pop(0)[...]
            y = jnp.dot(x, w_ref[...], preferred_element_type=F32)
            total = y if total is None else total + y
        refs[-1][...] = total.astype(BF16)

    depth = sum(b.shape[0] for b in rights)
    specs = [pl.BlockSpec(a.shape, lambda i, at: (0, 0)) for a in lefts + [whole]]
    specs += [pl.BlockSpec((b.shape[0], tile), lambda i, at: (0, i)) for b in rights]
    return pl.pallas_call(
        kernel,
        grid_spec=pltpu.PrefetchScalarGridSpec(
            num_scalar_prefetch=1,
            grid=(cols // tile,),
            in_specs=specs,
            out_specs=pl.BlockSpec((rows, tile), lambda i, at: (0, i)),
        ),
        out_shape=jax.ShapeDtypeStruct((rows, cols), BF16),
        compiler_params=pltpu.CompilerParams(
            dimension_semantics=("arbitrary",), vmem_limit_bytes=48 * 1024 * 1024
        ),
        cost_estimate=pl.CostEstimate(
            flops=2 * rows * cols * depth,
            bytes_accessed=2 * depth * (rows + cols) + 2 * rows * cols,
            transcendentals=0,
        ),
    )(places, *lefts, whole, *rights)


def input_grads(places, cot_t, grad, down, mine, other, nt, block_rows, begin):
    depth, rows = cot_t.shape
    part = mine.shape[0] // nt
    rank = grad.shape[1]
    step = math.gcd(block_rows, begin) if begin else block_rows
    whole_tile = step % 128 == 0

    def kernel(at, cot_ref, grad_ref, down_ref, mine_ref, other_ref, *outs):
        r = pl.program_id(0)
        for h, w_ref in enumerate((mine_ref, other_ref)):
            if whole_tile:
                start = pl.multiple_of(at[2 * nt + h] * block_rows + begin, 128)
                d = down_ref[:, pl.ds(start, part)]
            else:
                d = down_ref[h, 0]
            g = jnp.dot(w_ref[...], cot_ref[...], preferred_element_type=F32)
            g = g.T + jnp.dot(grad_ref[...], d, preferred_element_type=F32)
            for k in range(nt):

                @pl.when(r == k)
                def _(k=k, g=g, h=h):
                    outs[k][h] = g.astype(outs[k].dtype)

    if whole_tile:
        down_spec = pl.BlockSpec((rank, down.shape[1] // nt), lambda r, at: (0, at[nt + r]))
    else:
        cut = [
            lax.dynamic_slice(
                down.reshape(rank, nt, -1),
                (0, 0, places[2 * nt + h] * block_rows + begin),
                (rank, nt, part),
            )
            for h in range(2)
        ]
        down = jnp.stack(cut).transpose(0, 2, 1, 3)
        down_spec = pl.BlockSpec((2, 1, rank, part), lambda r, at: (0, at[nt + r], 0, 0))
    return pl.pallas_call(
        kernel,
        grid_spec=pltpu.PrefetchScalarGridSpec(
            num_scalar_prefetch=1,
            grid=(nt,),
            in_specs=[
                pl.BlockSpec((depth, rows), lambda r, at: (0, 0)),
                pl.BlockSpec((rows, rank), lambda r, at: (0, 0)),
                down_spec,
                pl.BlockSpec((part, depth), lambda r, at: (at[r], 0)),
                pl.BlockSpec((part, depth), lambda r, at: (at[r], 0)),
            ],
            out_specs=[pl.BlockSpec((2, rows, part), lambda r, at: (0, 0, 0))] * nt,
        ),
        out_shape=[
            jax.ShapeDtypeStruct((2, rows, part), F32 if k == 0 else BF16) for k in range(nt)
        ],
        compiler_params=pltpu.CompilerParams(
            dimension_semantics=("arbitrary",), vmem_limit_bytes=48 * 1024 * 1024
        ),
        cost_estimate=pl.CostEstimate(
            flops=4 * rows * (depth + rank) * mine.shape[0],
            bytes_accessed=2 * depth * (rows + 2 * mine.shape[0]) + 10 * rows * mine.shape[0],
            transcendentals=0,
        ),
    )(places, cot_t, grad, down, mine, other)


def gathered(x, n, bits):
    have = [(0, x)]
    size = x.shape[0]
    for b in bits:
        sent = jnp.concatenate([v for _, v in have], axis=0) if len(have) > 1 else x
        got = flip(sent, "fsdp", n, b)
        have = have + [
            (s | b, got[size * i : size * (i + 1)]) for i, (s, _) in enumerate(have)
        ]
    return dict(have)


def make_shards(nf, nt, nc):
    bits = [1 << k for k in range(nf.bit_length() - 1)]

    def shards(tokens, block_tenant_index, ranks, weight, down, up, cotangent):
        rows, local_d = tokens.shape
        local_f = cotangent.shape[1]
        own_tenants, largest_rank, _ = down.shape
        tenants = ranks.shape[0]
        block_rows = weight.shape[0]
        unit = block_rows // 5
        parts = (2 * unit, 2 * unit, block_rows - 4 * unit)
        begins = (0, 2 * unit, 4 * unit)
        pairs = len(parts)
        half_rank = largest_rank // 2
        f = lax.axis_index("fsdp")
        j = lax.axis_index("tenant")
        c = lax.axis_index("dp")

        row_tenant = jnp.broadcast_to(
            block_tenant_index[:, None], (block_tenant_index.shape[0], BLOCK)
        ).reshape(rows, 1)
        tenant_ids = jnp.arange(tenants, dtype=jnp.int32)[None, :]
        row_rank = jnp.sum(
            jnp.where(row_tenant == tenant_ids, ranks[None, :], 0), axis=1, keepdims=True
        )
        slots = jnp.arange(largest_rank, dtype=jnp.int32)[None, :]
        gain = jnp.where(slots < row_rank, alpha_scale / row_rank.astype(F32), F32(0.0))

        w_mine = []
        for p in range(pairs):
            half = parts[p] // 2
            got = [
                gathered(
                    weight[begins[p] + half * q : begins[p] + half * (q + 1)],
                    nf,
                    bits[::-1] if q else bits,
                )
                for q in range(2)
            ]
            w_mine.append(
                jnp.concatenate([got[q][s] for s in range(nf) for q in range(2)], axis=0)
            )
        w_other = [flip(w, "dp", nc, 1) for w in w_mine]

        def up_block(r):
            return lax.dynamic_slice(
                up, (0, c * half_rank, (j ^ r) * local_f), (own_tenants, half_rank, local_f)
            ).reshape(own_tenants * half_rank, local_f)

        up_mine = jnp.concatenate(
            [up_block(0)]
            + [flip(up_block(r), "tenant", nt, r) for r in range(1, nt)],
            axis=0,
        )
        up_other = flip(up_mine, "dp", nc, 1)

        def down_block(r):
            return lax.dynamic_slice(
                down, (0, c * half_rank, (j ^ r) * local_d), (own_tenants, half_rank, local_d)
            ).reshape(own_tenants * half_rank, local_d)

        down_mine = jnp.concatenate(
            [down_block(0)]
            + [flip(down_block(r), "tenant", nt, r) for r in range(1, nt)],
            axis=0,
        )
        down_other = flip(down_mine, "dp", nc, 1)

        tiles = [tokens] + [flip(tokens, "tenant", nt, r) for r in range(1, nt)]
        whole = lax.dynamic_update_slice(
            jnp.zeros((rows, nf * local_d), BF16), tokens, (0, (f ^ j) * local_d)
        )
        for r in range(1, nt):
            whole = lax.dynamic_update_slice(whole, tiles[r], (0, (f ^ j ^ r) * local_d))
        own_down = down.reshape(own_tenants * largest_rank, -1)
        cores = (c, c ^ 1)

        def columns(x, h, p):
            return jnp.concatenate(
                [
                    lax.dynamic_slice(
                        x,
                        (0, s * local_d + cores[h] * block_rows + begins[p]),
                        (x.shape[0], parts[p]),
                    )
                    for s in range(nf)
                ],
                axis=1,
            )

        def halves(x):
            a, b = x[:, :half_rank], x[:, half_rank:]
            return jnp.where(c == 0, x, jnp.concatenate([b, a], axis=1))

        def fold(x):
            total = jnp.zeros((rows, half_rank), F32)
            for r in range(nt):
                for l in range(own_tenants):
                    at = (r * own_tenants + l) * half_rank
                    t = (j ^ r) * own_tenants + l
                    total = total + jnp.where(row_tenant == t, x[:, at : at + half_rank], 0.0)
            return total

        def line_sum(x):
            got = [flip(x, "tenant", nt, r) for r in range(1, nt)]
            for g in got:
                x = x + g
            return x

        products = [dot(cotangent, u, 1, 1) for u in (up_mine, up_other)]
        products += [dot(tokens, d, 1, 1) for d in (down_mine, down_other)]
        mixed = line_sum(jnp.concatenate([fold(x) for x in products], axis=1))
        adapted_grad = (halves(mixed[:, :largest_rank]) * gain).astype(BF16)
        adapted = (halves(mixed[:, largest_rank:]) * gain).astype(BF16)

        def spread(x, ids):
            return jnp.concatenate([jnp.where(row_tenant == t, x, BF16(0.0)) for t in ids], axis=1)

        share = tenants // nc
        mine_ids = [c * share + k for k in range(share)]
        other_ids = [(c ^ 1) * share + k for k in range(share)]

        grad_mine = spread(adapted_grad, mine_ids)
        grad_other = spread(adapted_grad, other_ids)
        grad_own = spread(
            adapted_grad, [j * own_tenants + l for l in range(own_tenants)]
        )

        def core_share(small_mine, small_other, wide):
            other = dot(small_other, wide, 0, 0)
            return dot(small_mine, wide, 0, 0) + flip(other, "dp", nc, 1)

        down_share = core_share(grad_mine, grad_other, tokens)
        adapted_mine = spread(adapted, mine_ids)
        adapted_other = spread(adapted, other_ids)
        up_share = core_share(adapted_mine, adapted_other, cotangent)
        size = share * largest_rank // nf

        def share_piece(r):
            return jnp.concatenate(
                [
                    lax.dynamic_slice(x, ((f ^ r) * size, 0), (size, x.shape[1]))
                    for x in (down_share, up_share)
                ],
                axis=1,
            )

        got = [flip(share_piece(r).astype(BF16), "fsdp", nf, r) for r in range(1, nf)]
        mine = share_piece(0)
        for g in got:
            mine = mine + g.astype(F32)
        mine = mine.astype(BF16)
        blocks = [mine] + [flip(mine, "fsdp", nf, r) for r in range(1, nf)]

        def in_order(at, width):
            both = jnp.stack([x[:, at : at + width] for x in blocks])
            both = both.reshape((2,) * len(bits) + both.shape[1:])
            for k, b in enumerate(bits[::-1]):
                both = jnp.where((f & b) != 0, jnp.flip(both, k), both)
            return both.reshape(share, largest_rank, width).astype(F32)

        grad_down = in_order(0, local_d)
        grad_up = in_order(local_d, local_f)

        cotangent_t = cotangent.T
        places = jnp.stack(
            [f ^ j ^ r for r in range(nt)] + [j ^ r for r in range(nt)] + list(cores)
        ).astype(jnp.int32)
        out = [[], []]
        for p in range(pairs):
            own_part, *away = input_grads(
                places, cotangent_t, grad_own, own_down, w_mine[p], w_other[p],
                nt, block_rows, begins[p],
            )
            got = [flip(away[r - 1], "tenant", nt, r) for r in range(1, nt)]
            total = own_part
            for g in got:
                total = total + g.astype(F32)
            for h in range(2):
                out[h].append(total[h].astype(BF16))
        own, other = (jnp.concatenate(o, axis=1) for o in out)
        grad_tokens = jnp.where(
            c == 0,
            jnp.concatenate([own, other], axis=1),
            jnp.concatenate([other, own], axis=1),
        )

        ids = [(j ^ r) * own_tenants + l for r in range(nt) for l in range(own_tenants)]
        ordered = halves(adapted)
        terms = [
            (spread(ordered[:, :half_rank], ids), up_mine),
            (spread(ordered[:, half_rank:], ids), up_other),
        ]
        inside_kernel = math.gcd(block_rows, *begins) % 128 == 0
        for p in range(pairs):
            for h, w in enumerate((w_mine[p], w_other[p])):
                terms.append((None if inside_kernel else columns(whole, h, p), w))
        hidden = hidden_sum(
            jnp.stack(cores).astype(jnp.int32), whole, begins, block_rows, nf, terms
        )
        return hidden, grad_tokens, grad_down, grad_up

    return shards


def solution(mesh):
    nf, nt, nc = mesh.shape["fsdp"], mesh.shape["tenant"], mesh.shape["dp"]
    return jax.shard_map(
        make_shards(nf, nt, nc),
        mesh=mesh,
        in_specs=(
            P(("fsdp", "dp"), "tenant"),
            P(("fsdp", "dp")),
            P(),
            P(("fsdp", "dp"), "tenant"),
            P("tenant", None, None),
            P("tenant", None, None),
            P(("fsdp", "dp"), "tenant"),
        ),
        out_specs=(
            P(("fsdp", "dp"), "tenant"),
            P(("fsdp", "dp"), "tenant"),
            P("dp", None, "tenant"),
            P("dp", None, "tenant"),
        ),
        check_vma=False,
    )
```
